256 devices in a mesh: gx: 32 (over z, x), gy: 8 (over y, core).
Axes of the slice: x: 4, y: 4, z: 8, core: 2. Of those that a mesh axis runs over, the one named last changes fastest.
Arguments:
- orbitals: bfloat16 [20000, 200], P('gx'), may hold values from -6 to 6
- projector: bfloat16 [6016, 20000], P('gy', 'gx'), may hold values from -0.0390625 to 0.0390625
- integrals: bfloat16 [32, 6016, 6016], P('gx', 'gy'), may hold values from -1 to 1
Outputs:
- exchange_matrix: float32 [6016, 6016], P('gx', 'gy')
- exchange_orbitals: float32 [20000, 200], P('gx', 'gy')
- energy_mean: float32 [], replicated
- trace_mean: float32 [], replicated
The draws below stay inside these ranges and needn't reach their ends.
All inputs are finite; a program needn't handle non-finite values.
Results may differ from the reference program's by a relative error of at most 0.008.
Values may be sent and summed in bfloat16 or wider, within the bound.
A program may use at most 128 MiB of HBM per device.

```python
import jax
import jax.numpy as jnp
from jax import lax

NAO = 20000
NADM = 6016
NOCC = 200
NAUX = 32


def draw_integrals(key, part):
    keyed = jax.random.fold_in(key, 11)
    first = jax.random.fold_in(keyed, 0)
    shape = (NAUX, NADM, NADM)
    base = jax.random.normal(first, shape, jnp.float32)
    aux_scale = 0.5 + jnp.arange(NAUX, dtype=jnp.float32) / max(NAUX - 1, 1)
    row_scale = 0.5 + jnp.arange(NADM, dtype=jnp.float32) / max(NADM - 1, 1)
    sigma = (NADM * NOCC * NAUX) ** (-0.5)
    values = base * aux_scale[:, None, None] * row_scale[None, :, None] * sigma
    return jnp.clip(values, -1.0, 1.0).astype(jnp.bfloat16)


def block_scale(rng, shape, cuts, smallest, high):
    factor_of, own = 1.0, jax.random.fold_in(rng, 6)
    for axis_at, blocks in cuts:
        heights = jnp.exp(jax.random.uniform(jax.random.fold_in(own, axis_at), (blocks,), jnp.float32, smallest / len(cuts), high / len(cuts)))
        factor_of = factor_of * jnp.repeat(heights, shape[axis_at] // blocks).reshape([-1 if axis == axis_at else 1 for axis in range(len(shape))])
    return factor_of


def gaussian(rng, dims, width, reach, pieces=(), kind=jnp.bfloat16):
    gain = block_scale(rng, dims, pieces, -0.22, 0.18) if pieces else 1.0
    drawn = jax.random.normal(rng, dims, jnp.float32) * width * gain
    return jnp.minimum(jnp.maximum(drawn, -reach), reach).astype(kind)


def setup_inputs(seed: int = 0) -> dict:
    splits = jax.random.split(jax.random.key(seed), 4)
    return {
        "orbitals": gaussian(splits[0], (NAO, NOCC), 1.0, 6.0, ((0, 32),)),
        "projector": gaussian(splits[1], (NADM, NAO), NAO ** -0.5, 0.0390625, ((0, 8), (1, 32))),
        "integrals": draw_integrals(jax.random.fold_in(splits[3], 71), 0),
    }


def reference(orbitals, projector, integrals):
    admm = jnp.dot(projector, orbitals, preferred_element_type=jnp.float32).astype(jnp.bfloat16)

    def transform(slab):
        return jnp.dot(slab, admm, preferred_element_type=jnp.float32).astype(jnp.bfloat16)

    half = lax.map(transform, integrals)
    merged = jnp.transpose(half, (1, 0, 2)).reshape(NADM, NAUX * NOCC)
    exchange = jnp.dot(merged, merged.T, preferred_element_type=jnp.float32)
    admm_wide = admm.astype(jnp.float32)
    applied = jnp.dot(exchange, admm_wide, precision=lax.Precision.HIGHEST)
    applied_low = applied.astype(jnp.bfloat16)
    back = jnp.dot(projector.T, applied_low, preferred_element_type=jnp.float32)
    energy = -0.5 * jnp.sum(admm_wide * applied) / (NADM * NOCC)
    trace = jnp.sum(jnp.diagonal(exchange)) / NADM
    return exchange, back, energy, trace
```

```python
import functools

import jax
import jax.numpy as jnp
from jax import lax
from jax.experimental import pallas as pl
from jax.experimental.pallas import tpu as pltpu
from jax.sharding import PartitionSpec as P

MESH = pl.DeviceIdType.MESH
F32, BF16 = jnp.float32, jnp.bfloat16
NZ, NX, NY, NC = 8, 4, 4, 2
NG = NY * NC
PIECES = 6


def dot(a, b, ca, cb):
    return lax.dot_general(a, b, (((ca,), (cb,)), ((), ())), preferred_element_type=F32)


class Links:
    def __init__(self, send_sems, recv_sems, partner):
        self.send_sems, self.recv_sems, self.partner = send_sems, recv_sems, partner
        self.n_send = self.n_recv = 0
        self.pending = []

    def slot(self):
        self.n_recv += 1
        return self.n_recv - 1

    def send(self, src, dst, device, slot, pred=None):
        copy = pltpu.make_async_remote_copy(
            src_ref=src,
            dst_ref=dst,
            send_sem=self.send_sems.at[self.n_send],
            recv_sem=self.recv_sems.at[slot],
            device_id=device,
            device_id_type=MESH,
        )
        self.n_send += 1
        self.pending.append((copy, pred))
        if pred is None:
            copy.start()
        else:
            pl.when(pred)(copy.start)

    def arrived(self, dst, slot, pred=None):
        copy = pltpu.make_async_remote_copy(
            src_ref=dst,
            dst_ref=dst,
            send_sem=self.send_sems.at[0],
            recv_sem=self.recv_sems.at[slot],
            device_id=self.partner,
            device_id_type=MESH,
        )
        if pred is None:
            copy.wait_recv()
        else:
            pl.when(pred)(copy.wait_recv)

    def drain(self):
        for copy, pred in self.pending:
            if pred is None:
                copy.wait_send()
            else:
                pl.when(pred)(copy.wait_send)
        self.pending = []


def interleave(*flows):
    flows = list(flows)
    while flows:
        for flow in list(flows):
            try:
                next(flow)
            except StopIteration:
                flows.remove(flow)


def kernel(
    orb_ref,
    proj_ref,
    int_ref,
    exch_ref,
    back_ref,
    scal_ref,
    iv,
    pp,
    part,
    xs,
    xr,
    zs,
    zr,
    stage,
    full,
    hf,
    h16,
    hp,
    hh,
    acc,
    psend,
    prcv,
    ts,
    tr,
    tfull,
    dxs,
    dxr,
    dzs,
    dzr,
    ap,
    bk,
    bkr,
    sc,
    sr1,
    sr2,
    sr3,
    send_sems,
    recv_sems,
    int_sem,
):
    gx, gy = lax.axis_index("gx"), lax.axis_index("gy")
    z, x = gx // NX, gx % NX
    y, c = gy // NC, gy % NC
    rows = proj_ref.shape[0]
    npri = proj_ref.shape[1]
    nocc = orb_ref.shape[1]
    out_rows = rows // NX

    load = pltpu.make_async_copy(int_ref.at[0], iv, int_sem)
    load.start()

    def at(dz=0, dx=0, dy=0, dg=0):
        zz, xx = (z + dz) % NZ, (x + dx) % NX
        if dg:
            gg = (gy + dg) % NG
        else:
            gg = ((y + dy) % NY) * NC + c
        return (zz * NX + xx, gg)

    partner = (gx, y * NC + (1 - c))
    links = Links(send_sems, recv_sems, partner)

    barrier = pltpu.get_barrier_semaphore()
    peers = [at(dz=d) for d in range(1, NZ)] + [at(dx=d) for d in range(1, NX)]
    peers += [at(dg=d) for d in range(1, NG)]
    for peer in peers:
        pl.semaphore_signal(barrier, inc=1, device_id=peer, device_id_type=MESH)

    pp[...] = jnp.zeros_like(pp)
    pp[0:rows, 0:npri] = proj_ref[...]
    part[...] = jnp.zeros_like(part)
    part[0:rows, 0:nocc] = dot(proj_ref[...], orb_ref[...], 1, 0)
    hf[...] = jnp.zeros_like(hf)
    hp[...] = jnp.zeros_like(hp)
    bk[...] = jnp.zeros_like(bk)
    pl.semaphore_wait(barrier, len(peers))

    def ring4(dim, whole, halves, on_arrival=None):
        me = {"x": x, "y": y}[dim]
        step = (lambda d: at(dx=d)) if dim == "x" else (lambda d: at(dy=d))
        a, b, o0, o1 = links.slot(), links.slot(), links.slot(), links.slot()
        left, right, far = (me + 3) % 4, (me + 1) % 4, (me + 2) % 4
        links.send(whole(me), whole(me), step(1), a)
        links.send(whole(me), whole(me), step(3), b)
        yield
        links.arrived(whole(left), a)
        links.send(halves(left, 0), halves(left, 0), step(1), o0)
        if on_arrival:
            on_arrival(whole, left)
        yield
        links.arrived(whole(right), b)
        links.send(halves(right, 1), halves(right, 1), step(3), o1)
        if on_arrival:
            on_arrival(whole, right)
        yield
        links.arrived(halves(far, 0), o0)
        links.arrived(halves(far, 1), o1)
        if on_arrival:
            on_arrival(whole, far)

    def reduce_xz(src_ref, xs, xr, zs, zr, piece):
        xs[...] = src_ref[...].astype(BF16)
        slots = [links.slot() for _ in range(1, NX)]
        for d in range(1, NX):
            to = (x + d) % NX
            links.send(xs.at[pl.ds(to * 192, 192), :], xr.at[d - 1], at(dx=d), slots[d - 1])
        yield
        total = src_ref[pl.ds(x * 192, 192), :]
        for d in range(1, NX):
            links.arrived(xr.at[d - 1], slots[d - 1])
            total = total + xr[d - 1].astype(F32)
        src_ref[pl.ds(x * 192, 192), :] = total
        zs[...] = total.astype(BF16)
        slots = [links.slot() for _ in range(1, NZ)]
        for d in range(1, NZ):
            to = (z + d) % NZ
            first = jnp.minimum(to, PIECES - 1) * 32
            links.send(zs.at[pl.ds(first, 32), :], zr.at[d - 1], at(dz=d), slots[d - 1], to < PIECES)
        yield
        owner = z < PIECES
        for d in range(1, NZ):
            links.arrived(zr.at[d - 1], slots[d - 1], owner)

        own = jnp.minimum(z, PIECES - 1)

        @pl.when(owner)
        def _():
            total = src_ref[pl.ds(x * 192 + own * 32, 32), :]
            for d in range(1, NZ):
                total = total + zr[d - 1].astype(F32)
            piece(x, own)[...] = total.astype(BF16)

        slots = [links.slot() for _ in range(1, NZ)]
        for d in range(1, NZ):
            links.send(piece(x, own), piece(x, own), at(dz=d), slots[d - 1], owner)
        yield
        for d in range(1, NZ):
            src = (z + NZ - d) % NZ
            links.arrived(piece(x, jnp.minimum(src, PIECES - 1)), slots[d - 1], src < PIECES)

    def to_partner_y(blocks):
        def go(whole, i):
            slot = links.slot()
            links.send(whole(i), whole(i), partner, slot)
            core_waits.append((blocks, i, slot))

        return go

    core_waits = []
    interleave(
        reduce_xz(part, xs, xr, zs, zr, lambda i, k: stage.at[y, c, i, pl.ds(k * 32, 32), :])
    )
    interleave(
        ring4("x", lambda i: stage.at[y, c, i, 0:96, :], lambda i, h: stage.at[y, c, i, 48 * h : 48 * h + 48, :]),
        ring4("y", lambda i: stage.at[i, c, x, 96:192, :], lambda i, h: stage.at[i, c, x, 96 + 48 * h : 144 + 48 * h, :]),
    )
    low = lambda i: stage.at[i, c, :, 0:96, :]
    high = lambda i: stage.at[:, c, i, 96:192, :]
    low_other = lambda i: stage.at[i, 1 - c, :, 0:96, :]
    high_other = lambda i: stage.at[:, 1 - c, i, 96:192, :]
    to_partner_y(low_other)(low, y)
    to_partner_y(high_other)(high, x)
    interleave(
        ring4("y", low, lambda i, h: stage.at[i, c, 2 * h : 2 * h + 2, 0:96, :], to_partner_y(low_other)),
        ring4("x", high, lambda i, h: stage.at[2 * h : 2 * h + 2, c, i, 96:192, :], to_partner_y(high_other)),
    )
    for other, i, slot in core_waits:
        links.arrived(other(i), slot)
    for a in range(NY):
        for b in range(NC):
            for k in range(NX):
                n = min(192, rows - 192 * k)
                r0 = rows * (a * NC + b) + 192 * k
                full[r0 : r0 + n, :] = stage[a, b, k, 0:n, :]

    load.wait()
    for r0 in range(0, rows, 256):
        n = min(256, rows - r0)
        hf[r0 : r0 + n, :] = dot(iv[r0 : r0 + n, :], full[...], 1, 0)
    h16[...] = hf[...].astype(BF16)
    hr = h16[...].astype(F32)
    trace = jnp.sum(hr * hr)
    for k in range(NX):
        hp[192 * k : 192 * k + out_rows, :] = hf[out_rows * k : out_rows * (k + 1), :]
    hh[0, 0] = jnp.transpose(hp[...])[0:208, :].astype(BF16)

    ys, cs = z // NC, z % NC
    dy = (y + NY - ys) % NY
    on = c == cs
    is_src = on & (dy == 0)
    not_src = jnp.logical_not(is_src)
    is_next, is_prev = on & (dy == 1), on & (dy == 3)
    relay = on & (dy != 0)
    lhs_at = jnp.where(is_src, 0, 1)
    up, down, yup, ydown = at(dz=1), at(dz=NZ - 1), at(dy=1), at(dy=NY - 1)

    def half_of(which, s, h):
        return hh.at[which, s, :, 384 * h : 384 * h + 384]

    def flow_exchange():
        col_slots = {(s, h): links.slot() for s in range(1, NZ) for h in range(2)}
        row_slots = {(s, h): links.slot() for s in range(NZ) for h in range(2)}

        def spread(s, h):
            src, dst = half_of(0, s, h), half_of(1, s, h)
            for device in (yup, ydown, partner):
                links.send(src, dst, device, row_slots[s, h], is_src)

        def rows_in(s):
            for h in range(2):
                blk = half_of(1, s, h)
                links.arrived(blk, row_slots[s, h], not_src)
                if h == 0:
                    links.send(blk, blk, yup, row_slots[s, h], is_next)
                else:
                    links.send(blk, blk, ydown, row_slots[s, h], is_prev)
                links.send(blk, blk, partner, row_slots[s, h], relay)

        def accumulate(s, first=False):
            @pl.loop(0, 6)
            def _(m):
                cols = pl.ds(pl.multiple_of(m * 128, 128), 128)
                value = dot(hh[lhs_at, s, :, cols], hh[0, s], 0, 0)
                if first:
                    acc[cols, :] = value
                else:
                    acc[cols, :] += value

        for h in range(2):
            links.send(half_of(0, 0, h), half_of(0, 1, h), up, col_slots[1, h])
            links.send(half_of(0, 0, 1 - h), half_of(0, 7, 1 - h), down, col_slots[7, 1 - h])
        for h in range(2):
            spread(0, h)
        yield
        ready = [0]
        for k in (1, 2, 3):
            for j in range(2):
                h = j
                links.arrived(half_of(0, k, h), col_slots[k, h])
                if k < 3 or h == 0:
                    links.send(half_of(0, k, h), half_of(0, k + 1, h), up, col_slots[k + 1, h])
                spread(k, h)
                h = 1 - j
                links.arrived(half_of(0, 8 - k, h), col_slots[8 - k, h])
                if k < 3 or h == 1:
                    links.send(half_of(0, 8 - k, h), half_of(0, 7 - k, h), down, col_slots[7 - k, h])
                spread(8 - k, h)
            yield
            for s in ready:
                rows_in(s)
                accumulate(s, s == 0)
            ready = [k, 8 - k]
            yield
        for h in range(2):
            links.arrived(half_of(0, 4, h), col_slots[4, h])
            spread(4, h)
        yield
        for s in ready + [4]:
            rows_in(s)
            accumulate(s)
        slots = [links.slot() for _ in range(1, NX)]
        psend[...] = acc[...].astype(BF16)
        for d in range(1, NX):
            to = (x + d) % NX
            links.send(psend.at[pl.ds(to * 192, 192), :], prcv.at[d - 1], at(dx=d), slots[d - 1])
        yield
        total = acc[pl.ds(x * 192, 192), :]
        for d in range(1, NX):
            links.arrived(prcv.at[d - 1], slots[d - 1])
            total = total + prcv[d - 1].astype(F32)
        lane = lax.broadcasted_iota(jnp.int32, total.shape, 1)
        out = total
        for k in range(1, NX):
            moved = pltpu.roll(total, total.shape[1] - 4 * k, 1)
            out = jnp.where(lane >= out_rows * k, moved, out)
        exch_ref[...] = out[0:out_rows, 0:rows]

    def flow_applied():
        own = stage[y, c].reshape(4 * 192, 256)
        tt = dot(own, h16[...], 0, 0).astype(BF16)
        share = nocc // NG
        r = lax.broadcasted_iota(jnp.int32, (256, 256), 0)
        j = lax.broadcasted_iota(jnp.int32, (256, 256), 1)
        pick = ((r % 32 < share) & (j == share * (r // 32) + r % 32)).astype(F32).astype(BF16)
        ts[...] = dot(pick, tt, 1, 0).astype(BF16)
        slots = [links.slot() for _ in range(1, NG)]
        for d in range(1, NG):
            to = (gy + d) % NG
            links.send(ts.at[pl.ds(to * 32, 32), :], tr.at[d - 1], at(dg=d), slots[d - 1])
        yield
        total = ts[pl.ds(gy * 32, 32), :].astype(F32)
        for d in range(1, NG):
            links.arrived(tr.at[d - 1], slots[d - 1])
            total = total + tr[d - 1].astype(F32)
        energy = jnp.sum(total * total)
        tfull[pl.ds(gy * 32, 32), :] = total.astype(BF16)
        slots = [links.slot() for _ in range(1, NG)]
        s1 = [links.slot() for _ in range(1, NG)]
        mine = tfull.at[pl.ds(gy * 32, 32), :]
        sc[0] = jnp.where(lax.broadcasted_iota(jnp.int32, (8, 128), 0) == 0, trace, energy)
        for d in range(1, NG):
            links.send(mine, mine, at(dg=d), slots[d - 1])
            links.send(sc.at[0], sr1.at[d - 1], at(dg=d), s1[d - 1])
        yield
        for d in range(1, NG):
            src = (gy + NG - d) % NG
            links.arrived(tfull.at[pl.ds(src * 32, 32), :], slots[d - 1])
        part[...] = dot(h16[...], tfull[...], 1, 1)
        total = sc[0]
        for d in range(1, NG):
            links.arrived(sr1.at[d - 1], s1[d - 1])
            total = total + sr1[d - 1]
        sc[1] = total
        s2 = [links.slot() for _ in range(1, NX)]
        for d in range(1, NX):
            links.send(sc.at[1], sr2.at[d - 1], at(dx=d), s2[d - 1])
        for _ in reduce_xz(part, dxs, dxr, dzs, dzr, lambda i, k: ap.at[i, pl.ds(k * 32, 32), :]):
            yield
        total = sc[1]
        for d in range(1, NX):
            links.arrived(sr2.at[d - 1], s2[d - 1])
            total = total + sr2[d - 1]
        sc[2] = total
        s3 = [links.slot() for _ in range(1, NZ)]
        for d in range(1, NZ):
            links.send(sc.at[2], sr3.at[d - 1], at(dz=d), s3[d - 1])
        for _ in ring4("x", lambda i: ap.at[i], lambda i, h: ap.at[i, 96 * h : 96 * h + 96, :]):
            yield
        bt = dot(ap[...].reshape(4 * 192, 256), pp[...], 0, 0)
        bk[...] = bt.astype(BF16)
        slots = [links.slot() for _ in range(1, NG)]
        for d in range(1, NG):
            to = (gy + d) % NG
            links.send(bk.at[pl.ds(to * 32, 32), :], bkr.at[d - 1], at(dg=d), slots[d - 1])
        yield
        total = bk[pl.ds(gy * 32, 32), :].astype(F32)
        for d in range(1, NG):
            links.arrived(bkr.at[d - 1], slots[d - 1])
            total = total + bkr[d - 1].astype(F32)
        back_ref[...] = total
        total = sc[2]
        for d in range(1, NZ):
            links.arrived(sr3.at[d - 1], s3[d - 1])
            total = total + sr3[d - 1]
        scal_ref[...] = total

    interleave(flow_exchange(), flow_applied())
    links.drain()


N_SEMS = 320


def on_device(orbitals, projector, integrals):
    rows, npri = projector.shape
    total_adm = integrals.shape[2]
    nocc = orbitals.shape[1]
    out_rows = rows // NX
    vmem = pl.BlockSpec(memory_space=pltpu.VMEM)
    scratch = [
        pltpu.VMEM((rows, total_adm), BF16),
        pltpu.VMEM((768, 640), BF16),
        pltpu.VMEM((768, 256), F32),
        pltpu.VMEM((768, 256), BF16),
        pltpu.VMEM((3, 192, 256), BF16),
        pltpu.VMEM((192, 256), BF16),
        pltpu.VMEM((7, 32, 256), BF16),
        pltpu.VMEM((NY, NC, NX, 192, 256), BF16),
        pltpu.VMEM((total_adm, 256), BF16),
        pltpu.VMEM((768, 256), F32),
        pltpu.VMEM((768, 256), BF16),
        pltpu.VMEM((768, 256), F32),
        pltpu.VMEM((2, NZ, 208, 768), BF16),
        pltpu.VMEM((768, 768), F32),
        pltpu.VMEM((768, 768), BF16),
        pltpu.VMEM((3, 192, 768), BF16),
        pltpu.VMEM((256, 256), BF16),
        pltpu.VMEM((7, 32, 256), BF16),
        pltpu.VMEM((256, 256), BF16),
        pltpu.VMEM((768, 256), BF16),
        pltpu.VMEM((3, 192, 256), BF16),
        pltpu.VMEM((192, 256), BF16),
        pltpu.VMEM((7, 32, 256), BF16),
        pltpu.VMEM((NX, 192, 256), BF16),
        pltpu.VMEM((256, 640), BF16),
        pltpu.VMEM((7, 32, 640), BF16),
        pltpu.VMEM((3, 8, 128), F32),
        pltpu.VMEM((7, 8, 128), F32),
        pltpu.VMEM((3, 8, 128), F32),
        pltpu.VMEM((7, 8, 128), F32),
        pltpu.SemaphoreType.DMA((N_SEMS,)),
        pltpu.SemaphoreType.DMA((N_SEMS,)),
        pltpu.SemaphoreType.DMA,
    ]
    exchange, back, scal = pl.pallas_call(
        kernel,
        out_shape=(
            jax.ShapeDtypeStruct((out_rows, rows), F32),
            jax.ShapeDtypeStruct((32, 640), F32),
            jax.ShapeDtypeStruct((8, 128), F32),
        ),
        in_specs=[vmem, vmem, pl.BlockSpec(memory_space=pl.ANY)],
        out_specs=(vmem, vmem, vmem),
        scratch_shapes=scratch,
        compiler_params=pltpu.CompilerParams(
            collective_id=0, has_side_effects=True, vmem_limit_bytes=56 * 1024 * 1024
        ),
        name="admm_exchange",
    )(orbitals, projector, integrals)
    trace_mean = scal[0, 0] / total_adm
    energy_mean = -0.5 * scal[1, 0] / (total_adm * nocc)
    return exchange, back[0 : nocc // NG, 0:npri].T, energy_mean, trace_mean


def solution(mesh):
    return jax.shard_map(
        on_device,
        mesh=mesh,
        in_specs=(P("gx", None), P("gy", "gx"), P("gx", "gy", None)),
        out_specs=(P("gx", "gy"), P("gx", "gy"), P(), P()),
        check_vma=False,
    )
```

```python
import functools

import jax
import jax.numpy as jnp
from jax import lax
from jax.experimental import pallas as pl
from jax.experimental.pallas import tpu as pltpu
from jax.sharding import PartitionSpec as P

MESH = pl.DeviceIdType.MESH
F32, BF16 = jnp.float32, jnp.bfloat16
NZ, NX, NY, NC = 8, 4, 4, 2
NG = NY * NC
PIECES = 6


def dot(a, b, ca, cb):
    return lax.dot_general(a, b, (((ca,), (cb,)), ((), ())), preferred_element_type=F32)


LAG = 3
D_AT = [0,5,9,14,18,22,26,29,34]


class Links:
    def __init__(self, send_sems, recv_sems, partner):
        self.send_sems, self.recv_sems, self.partner = send_sems, recv_sems, partner
        self.n_send = self.n_recv = 0
        self.pending = []

    def slot(self):
        self.n_recv += 1
        return self.n_recv - 1

    def send(self, src, dst, device, slot, pred=None):
        copy = pltpu.make_async_remote_copy(
            src_ref=src,
            dst_ref=dst,
            send_sem=self.send_sems.at[self.n_send],
            recv_sem=self.recv_sems.at[slot],
            device_id=device,
            device_id_type=MESH,
        )
        self.n_send += 1
        self.pending.append((copy, pred))
        if pred is None:
            copy.start()
        else:
            pl.when(pred)(copy.start)

    def arrived(self, dst, slot, pred=None):
        copy = pltpu.make_async_remote_copy(
            src_ref=dst,
            dst_ref=dst,
            send_sem=self.send_sems.at[0],
            recv_sem=self.recv_sems.at[slot],
            device_id=self.partner,
            device_id_type=MESH,
        )
        if pred is None:
            copy.wait_recv()
        else:
            pl.when(pred)(copy.wait_recv)

    def drain(self):
        for copy, pred in self.pending:
            if pred is None:
                copy.wait_send()
            else:
                pl.when(pred)(copy.wait_send)
        self.pending = []


def together(*flows):
    flows = list(flows)
    while flows:
        for flow in list(flows):
            if next(flow, "end") == "end":
                flows.remove(flow)
        yield


def interleave(*flows):
    for _ in together(*flows):
        pass


def kernel(
    orb_ref,
    proj_ref,
    int_ref,
    exch_ref,
    back_ref,
    scal_ref,
    iv,
    pp,
    part,
    xs,
    xr,
    zs,
    zr,
    stage,
    full,
    hf,
    h16,
    hp,
    hh,
    acc,
    psend,
    prcv,
    ts,
    tr,
    tfull,
    dxs,
    dxr,
    dzs,
    dzr,
    ap,
    bk,
    bkr,
    sc,
    sr1,
    sr2,
    sr3,
    send_sems,
    recv_sems,
    int_sem,
):
    gx, gy = lax.axis_index("gx"), lax.axis_index("gy")
    z, x = gx // NX, gx % NX
    y, c = gy // NC, gy % NC
    rows = proj_ref.shape[0]
    npri = proj_ref.shape[1]
    nocc = orb_ref.shape[0]
    out_rows = rows // NX

    load = pltpu.make_async_copy(int_ref.at[0], iv, int_sem)
    load.start()

    def at(dz=0, dx=0, dy=0, dg=0):
        zz, xx = (z + dz) % NZ, (x + dx) % NX
        if dg:
            gg = (gy + dg) % NG
        else:
            gg = ((y + dy) % NY) * NC + c
        return (zz * NX + xx, gg)

    partner = (gx, y * NC + (1 - c))
    links = Links(send_sems, recv_sems, partner)

    barrier = pltpu.get_barrier_semaphore()
    peers = [at(dz=d) for d in range(1, NZ)] + [at(dx=d) for d in range(1, NX)]
    peers += [at(dg=d) for d in range(1, NG)]
    for peer in peers:
        pl.semaphore_signal(barrier, inc=1, device_id=peer, device_id_type=MESH)

    part[...] = jnp.zeros_like(part)
    share = dot(proj_ref[...], orb_ref[...], 1, 1)
    part[0, 0:rows, :] = share[:, 0:128]
    part[1, 0:rows, 0 : nocc - 128] = share[:, 128:nocc]
    pl.semaphore_wait(barrier, len(peers))

    def ring4(dim, part_of, on_arrival=None):
        me = {"x": x, "y": y}[dim]
        step = (lambda d: at(dx=d)) if dim == "x" else (lambda d: at(dy=d))
        left, right, far = (me + 3) % 4, (me + 1) % 4, (me + 2) % 4
        from_left, from_right, from_far = [[links.slot(), links.slot()] for _ in range(3)]

        def send(i, h, d, slots):
            links.send(part_of(i, h), part_of(i, h), step(d), slots[h])

        def arrived(i, h, slots):
            links.arrived(part_of(i, h), slots[h])

        def seen(i, h):
            if on_arrival:
                on_arrival(part_of, i, h)

        send(me, 0, 1, from_left)
        send(me, 1, 3, from_right)
        send(me, 1, 1, from_left)
        send(me, 0, 3, from_right)
        yield
        arrived(left, 0, from_left)
        send(left, 0, 1, from_far)
        arrived(right, 1, from_right)
        send(right, 1, 3, from_far)
        seen(left, 0)
        seen(right, 1)
        yield
        arrived(left, 1, from_left)
        arrived(right, 0, from_right)
        seen(left, 1)
        seen(right, 0)
        for h in range(2):
            arrived(far, h, from_far)
            seen(far, h)

    def direct4(dim, whole):
        me = {"x": x, "y": y}[dim]
        step = (lambda d: at(dx=d)) if dim == "x" else (lambda d: at(dy=d))
        slots = [links.slot() for _ in range(3)]
        for d in (2, 1, 3):
            links.send(whole(me), whole(me), step(d), slots[d - 1])
        yield
        for d in (1, 3, 2):
            links.arrived(whole((me + 4 - d) % 4), slots[d - 1])

    def reduce_xz(src_ref, xs, xr, zs, zr, piece, lanes):
        xs[lanes] = src_ref[lanes].astype(BF16)
        slots = [links.slot() for _ in range(1, NX)]
        for d in (2, 1, 3):
            to = (x + d) % NX
            links.send(xs.at[lanes, pl.ds(to * 192, 192)], xr.at[lanes, d - 1], at(dx=d), slots[d - 1])
        yield
        total = src_ref[lanes, pl.ds(x * 192, 192)]
        for d in (1, 3, 2):
            links.arrived(xr.at[lanes, d - 1], slots[d - 1])
            total = total + xr[lanes, d - 1].astype(F32)
        src_ref[lanes, pl.ds(x * 192, 192)] = total
        zs[lanes] = total.astype(BF16)
        slots = [links.slot() for _ in range(1, NZ)]
        for d in (4, 3, 5, 2, 6, 1, 7):
            to = (z + d) % NZ
            first = jnp.minimum(to, PIECES - 1) * 32
            links.send(zs.at[lanes, pl.ds(first, 32)], zr.at[lanes, d - 1], at(dz=d), slots[d - 1], to < PIECES)
        yield
        owner = z < PIECES
        for d in range(1, NZ):
            links.arrived(zr.at[lanes, d - 1], slots[d - 1], owner)

        own = jnp.minimum(z, PIECES - 1)

        @pl.when(owner)
        def _():
            total = src_ref[lanes, pl.ds(x * 192 + own * 32, 32)]
            for d in range(1, NZ):
                total = total + zr[lanes, d - 1].astype(F32)
            piece(x, own)[...] = total.astype(BF16)

        slots = [links.slot() for _ in range(1, NZ)]
        for d in (4, 3, 5, 2, 6, 1, 7):
            links.send(piece(x, own), piece(x, own), at(dz=d), slots[d - 1], owner)
        yield
        for d in range(1, NZ):
            src = (z + NZ - d) % NZ
            links.arrived(piece(x, jnp.minimum(src, PIECES - 1)), slots[d - 1], src < PIECES)

    def flow_admm(lanes):
        waits = []

        def to_partner(other):
            def go(part_of, i, h):
                slot = links.slot()
                links.send(part_of(i, h), part_of(i, h), partner, slot)
                waits.append((other, i, h, slot))

            return go

        yield from reduce_xz(part, xs, xr, zs, zr, lambda i, k: stage.at[lanes, y, c, i, pl.ds(k * 32, 32)], lanes)
        yield from together(
            direct4("x", lambda i: stage.at[lanes, y, c, i, 0:96]),
            direct4("y", lambda i: stage.at[lanes, i, c, x, 96:192]),
        )
        low = lambda i, h: stage.at[lanes, i, c, 2 * h : 2 * h + 2, 0:96]
        high = lambda i, h: stage.at[lanes, 2 * h : 2 * h + 2, c, i, 96:192]
        low_sent = to_partner(lambda i, h: stage.at[lanes, i, 1 - c, 2 * h : 2 * h + 2, 0:96])
        high_sent = to_partner(lambda i, h: stage.at[lanes, 2 * h : 2 * h + 2, 1 - c, i, 96:192])
        both = together(ring4("y", low, low_sent), ring4("x", high, high_sent))
        next(both)
        for h in range(2):
            low_sent(low, y, h)
            high_sent(high, x, h)
        yield
        yield from both
        for other, i, h, slot in waits:
            links.arrived(other(i, h), slot)

    def housekeeping():
        pp[...] = jnp.zeros_like(pp)
        pp[0:rows, 0:npri] = proj_ref[...]
        hf[...] = jnp.zeros_like(hf)
        hp[...] = jnp.zeros_like(hp)
        yield

    flows = [flow_admm(0), flow_admm(1)]
    interleave(*flows, housekeeping())
    for a in range(NY):
        for b in range(NC):
            for k in range(NX):
                n = min(192, rows - 192 * k)
                r0 = rows * (a * NC + b) + 192 * k
                full[r0 : r0 + n, 0:128] = stage[0, a, b, k, 0:n, :]
                full[r0 : r0 + n, 128:256] = stage[1, a, b, k, 0:n, :]

    load.wait()
    for r0 in range(0, rows, 256):
        n = min(256, rows - r0)
        hf[r0 : r0 + n, :] = dot(iv[r0 : r0 + n, :], full[...], 1, 0)
    h16[...] = hf[...].astype(BF16)
    hr = h16[...].astype(F32)
    trace = jnp.sum(hr * hr)
    for k in range(NX):
        hp[192 * k : 192 * k + out_rows, :] = hf[out_rows * k : out_rows * (k + 1), :]
    ht = jnp.transpose(hp[...])[0:208, :].astype(BF16)
    for j in range(6):
        hh[0, 0, j] = ht[:, 128 * j : 128 * j + 128]

    ys, cs = z // NC, z % NC
    dy = (y + NY - ys) % NY
    on = c == cs
    is_src = on & (dy == 0)
    lhs_at = jnp.where(is_src, 0, 1)
    up, down, yup, ydown = at(dz=1), at(dz=NZ - 1), at(dy=1), at(dy=NY - 1)

    def piece_of(which, s, j):
        return hh.at[which, s, j]

    def accumulate(s, first=False):
        @pl.loop(0, 6)
        def _(m):
            cols = pl.ds(pl.multiple_of(m * 128, 128), 128)
            value = dot(hh[lhs_at, s, m], jnp.concatenate([hh[0, s, j] for j in range(6)], 1), 0, 0)
            if first:
                acc[cols, :] = value
            else:
                acc[cols, :] += value

    def flow_exchange():
        col_slots = {(s, j): links.slot() for s in range(1, NZ) for j in range(6)}
        row_slots = {(s, j): links.slot() for s in range(NZ) for j in range(6)}
        pairs = {e - 2: [(0, e), (0, 5 - e)] for e in range(3)}
        for k in (1, 2, 3):
            for j in range(6):
                pairs[6 * k - 5 + j] = [(k, j), (8 - k, 5 - j)]
        for j in range(3):
            pairs[19 + j] = [(4, j), (4, 5 - j)]

        def pass_on(s, j):
            if s in (0, 1, 2) or (s == 3 and j < 3):
                links.send(piece_of(0, s, j), piece_of(0, s + 1, j), up, col_slots[s + 1, j])
            if s in (0, 7, 6) or (s == 5 and j >= 3):
                t = (s - 1) % 8
                links.send(piece_of(0, s, j), piece_of(0, t, j), down, col_slots[t, j])

        def spread(s, j):
            src, dst = piece_of(0, s, j), piece_of(1, s, j)
            links.send(src, dst, yup if j < 3 else ydown, row_slots[s, j], is_src)
            links.send(src, dst, partner, row_slots[s, j], is_src)

        def relay(s, j, h):
            blk = piece_of(1, s, j)
            here = on & (dy == (h if j < 3 else 4 - h))
            links.arrived(blk, row_slots[s, j], here)
            if h < 3:
                links.send(blk, blk, yup if j < 3 else ydown, row_slots[s, j], here)
            links.send(blk, blk, partner, row_slots[s, j], here)

        def finish_slot(s):
            for j in range(6):
                links.arrived(piece_of(1, s, j), row_slots[s, j], jnp.logical_not(on))
            accumulate(s, s == 0)

        for j in range(6):
            pass_on(0, [0, 5, 1, 4, 2, 3][j])
        yield
        for j in range(6):
            spread(0, [0, 5, 1, 4, 2, 3][j])
        yield
        last = 21 + 3 * LAG
        for e in range(0, last + 1):
            if 1 <= e <= 21:
                for s, j in pairs[e]:
                    links.arrived(piece_of(0, s, j), col_slots[s, j])
                    pass_on(s, j)
                    spread(s, j)
            for h in (1, 2, 3):
                for s, j in pairs.get(e - LAG * h, ()):
                    relay(s, j, h)
            q = e - 3 * LAG - 1
            if q == 0:
                finish_slot(0)
            elif q in (6, 12, 18):
                finish_slot(q // 6)
                finish_slot(8 - q // 6)
            yield
        finish_slot(4)
        slots = [links.slot() for _ in range(6)]
        left, right, far = (x + 3) % NX, (x + 1) % NX, (x + 2) % NX
        to_right, to_left = at(dx=1), at(dx=3)
        def mine(i, h):
            return acc[pl.ds(i * 192, 192), 384 * h : 384 * h + 384]

        psend[0] = mine(far, 0).astype(BF16)
        links.send(psend.at[0], prcv.at[0], to_right, slots[0])
        psend[1] = mine(far, 1).astype(BF16)
        links.send(psend.at[1], prcv.at[1], to_left, slots[1])
        psend[2] = mine(right, 1).astype(BF16)
        links.send(psend.at[2], prcv.at[2], to_right, slots[2])
        psend[3] = mine(left, 0).astype(BF16)
        links.send(psend.at[3], prcv.at[3], to_left, slots[3])
        yield
        links.arrived(prcv.at[0], slots[0])
        psend[4] = (mine(right, 0) + prcv[0].astype(F32)).astype(BF16)
        links.send(psend.at[4], prcv.at[4], to_right, slots[4])
        links.arrived(prcv.at[1], slots[1])
        psend[5] = (mine(left, 1) + prcv[1].astype(F32)).astype(BF16)
        links.send(psend.at[5], prcv.at[5], to_left, slots[5])
        yield
        for j in (2, 3, 4, 5):
            links.arrived(prcv.at[j], slots[j])
        first = mine(x, 0) + prcv[3].astype(F32) + prcv[4].astype(F32)
        second = mine(x, 1) + prcv[2].astype(F32) + prcv[5].astype(F32)
        total = jnp.concatenate([first, second], 1)
        lane = lax.broadcasted_iota(jnp.int32, total.shape, 1)
        out = total
        for k in range(1, NX):
            moved = pltpu.roll(total, total.shape[1] - 4 * k, 1)
            out = jnp.where(lane >= out_rows * k, moved, out)
        exch_ref[...] = out[0:out_rows, 0:rows]

    def flow_applied():
        own = jnp.concatenate([stage[i, y, c].reshape(4 * 192, 128) for i in range(2)], 1)
        tt = dot(own, h16[...], 0, 0).astype(BF16)
        share = nocc // NG
        r = lax.broadcasted_iota(jnp.int32, (256, 256), 0)
        j = lax.broadcasted_iota(jnp.int32, (256, 256), 1)
        pick = ((r % 32 < share) & (j == share * (r // 32) + r % 32)).astype(F32).astype(BF16)
        ts[...] = dot(pick, tt, 1, 0).astype(BF16)
        slots = [links.slot() for _ in range(1, NG)]
        for d in range(1, NG):
            to = (gy + d) % NG
            links.send(ts.at[pl.ds(to * 32, 32), :], tr.at[d - 1], at(dg=d), slots[d - 1])
        yield
        total = ts[pl.ds(gy * 32, 32), :].astype(F32)
        for d in range(1, NG):
            links.arrived(tr.at[d - 1], slots[d - 1])
            total = total + tr[d - 1].astype(F32)
        energy = jnp.sum(total * total)
        tfull[pl.ds(gy * 32, 32), :] = total.astype(BF16)
        slots = [links.slot() for _ in range(1, NG)]
        s1 = [links.slot() for _ in range(1, NG)]
        mine = tfull.at[pl.ds(gy * 32, 32), :]
        sc[0] = jnp.where(lax.broadcasted_iota(jnp.int32, (8, 128), 0) == 0, trace, energy)
        for d in range(1, NG):
            links.send(mine, mine, at(dg=d), slots[d - 1])
            links.send(sc.at[0], sr1.at[d - 1], at(dg=d), s1[d - 1])
        yield
        for d in range(1, NG):
            src = (gy + NG - d) % NG
            links.arrived(tfull.at[pl.ds(src * 32, 32), :], slots[d - 1])
        applied = dot(h16[...], tfull[...], 1, 1)
        part[0] = applied[:, 0:128]
        part[1] = applied[:, 128:256]
        total = sc[0]
        for d in range(1, NG):
            links.arrived(sr1.at[d - 1], s1[d - 1])
            total = total + sr1[d - 1]
        sc[1] = total
        s2 = [links.slot() for _ in range(1, NX)]
        for d in range(1, NX):
            links.send(sc.at[1], sr2.at[d - 1], at(dx=d), s2[d - 1])
        for _ in reduce_xz(part, dxs, dxr, dzs, dzr, lambda i, k: ap.at[:, i, pl.ds(k * 32, 32)], slice(0, 2)):
            yield
        total = sc[1]
        for d in range(1, NX):
            links.arrived(sr2.at[d - 1], s2[d - 1])
            total = total + sr2[d - 1]
        sc[2] = total
        s3 = [links.slot() for _ in range(1, NZ)]
        for d in range(1, NZ):
            links.send(sc.at[2], sr3.at[d - 1], at(dz=d), s3[d - 1])
        for _ in ring4("x", lambda i, h: ap.at[h, i]):
            yield
        whole = jnp.concatenate([ap[i].reshape(4 * 192, 128) for i in range(2)], 1)
        bt = dot(whole, pp[...], 0, 0)
        bk[...] = bt.astype(BF16)
        slots = [links.slot() for _ in range(1, NG)]
        for d in range(1, NG):
            to = (gy + d) % NG
            links.send(bk.at[pl.ds(to * 32, 32), :], bkr.at[d - 1], at(dg=d), slots[d - 1])
        yield
        total = bk[pl.ds(gy * 32, 32), :].astype(F32)
        for d in range(1, NG):
            links.arrived(bkr.at[d - 1], slots[d - 1])
            total = total + bkr[d - 1].astype(F32)
        back_ref[...] = total
        total = sc[2]
        for d in range(1, NZ):
            links.arrived(sr3.at[d - 1], s3[d - 1])
            total = total + sr3[d - 1]
        scal_ref[...] = total

    exchange, applied = flow_exchange(), flow_applied()
    for step, _ in enumerate(exchange):
        for _ in range(D_AT.count(step)):
            next(applied, None)
    for _ in applied:
        pass
    links.drain()


N_SEMS = 720


def finish(total_adm, nocc, exch_ref, back_ref, scal_ref, exch_out, back_out, energy_out, trace_out):
    exch_out[...] = exch_ref[...]
    back_out[...] = back_ref[0 : back_out.shape[0], 0 : back_out.shape[1]]
    trace_out[...] = scal_ref[0:1, 0:1] / total_adm
    energy_out[...] = -0.5 * scal_ref[1:2, 0:1] / (total_adm * nocc)


def on_device(orbitals, projector, integrals):
    rows, npri = projector.shape
    total_adm = integrals.shape[2]
    nocc = orbitals.shape[1]
    out_rows = rows // NX
    vmem = pl.BlockSpec(memory_space=pltpu.VMEM)
    scratch = [
        pltpu.VMEM((rows, total_adm), BF16),
        pltpu.VMEM((768, 640), BF16),
        pltpu.VMEM((2, 768, 128), F32),
        pltpu.VMEM((2, 768, 128), BF16),
        pltpu.VMEM((2, 3, 192, 128), BF16),
        pltpu.VMEM((2, 192, 128), BF16),
        pltpu.VMEM((2, 7, 32, 128), BF16),
        pltpu.VMEM((2, NY, NC, NX, 192, 128), BF16),
        pltpu.VMEM((total_adm, 256), BF16),
        pltpu.VMEM((768, 256), F32),
        pltpu.VMEM((768, 256), BF16),
        pltpu.VMEM((768, 256), F32),
        pltpu.VMEM((2, NZ, 6, 208, 128), BF16),
        pltpu.VMEM((768, 768), F32),
        pltpu.VMEM((6, 192, 384), BF16),
        pltpu.VMEM((6, 192, 384), BF16),
        pltpu.VMEM((256, 256), BF16),
        pltpu.VMEM((7, 32, 256), BF16),
        pltpu.VMEM((256, 256), BF16),
        pltpu.VMEM((2, 768, 128), BF16),
        pltpu.VMEM((2, 3, 192, 128), BF16),
        pltpu.VMEM((2, 192, 128), BF16),
        pltpu.VMEM((2, 7, 32, 128), BF16),
        pltpu.VMEM((2, NX, 192, 128), BF16),
        pltpu.VMEM((256, 640), BF16),
        pltpu.VMEM((7, 32, 640), BF16),
        pltpu.VMEM((3, 8, 128), F32),
        pltpu.VMEM((7, 8, 128), F32),
        pltpu.VMEM((3, 8, 128), F32),
        pltpu.VMEM((7, 8, 128), F32),
        pltpu.SemaphoreType.DMA((N_SEMS,)),
        pltpu.SemaphoreType.DMA((N_SEMS,)),
        pltpu.SemaphoreType.DMA,
    ]
    exchange, back, scal = pl.pallas_call(
        kernel,
        out_shape=(
            jax.ShapeDtypeStruct((out_rows, rows), F32),
            jax.ShapeDtypeStruct((32, 640), F32),
            jax.ShapeDtypeStruct((8, 128), F32),
        ),
        in_specs=[vmem, vmem, pl.BlockSpec(memory_space=pl.ANY)],
        out_specs=(vmem, vmem, vmem),
        scratch_shapes=scratch,
        compiler_params=pltpu.CompilerParams(
            collective_id=0, has_side_effects=True, vmem_limit_bytes=56 * 1024 * 1024
        ),
        name="admm_exchange",
    )(orbitals.T, projector, integrals)
    exchange, back, energy_mean, trace_mean = pl.pallas_call(
        functools.partial(finish, total_adm, nocc),
        out_shape=(
            jax.ShapeDtypeStruct((out_rows, rows), F32),
            jax.ShapeDtypeStruct((nocc // NG, npri), F32),
            jax.ShapeDtypeStruct((1, 1), F32),
            jax.ShapeDtypeStruct((1, 1), F32),
        ),
        in_specs=[vmem] * 3,
        out_specs=(vmem,) * 4,
        name="finish",
    )(exchange, back, scal)
    return exchange, back.T, energy_mean.reshape(()), trace_mean.reshape(())


def solution(mesh):
    return jax.shard_map(
        on_device,
        mesh=mesh,
        in_specs=(P("gx", None), P("gy", "gx"), P("gx", "gy", None)),
        out_specs=(P("gx", "gy"), P("gx", "gy"), P(), P()),
        check_vma=False,
    )
```

```python
import functools

import jax
import jax.numpy as jnp
from jax import lax
from jax.experimental import pallas as pl
from jax.experimental.pallas import tpu as pltpu
from jax.sharding import PartitionSpec as P

MESH = pl.DeviceIdType.MESH
F32, BF16 = jnp.float32, jnp.bfloat16
NZ, NX, NY, NC = 8, 4, 4, 2
NG = NY * NC
PIECES = 6


def dot(a, b, ca, cb):
    return lax.dot_general(a, b, (((ca,), (cb,)), ((), ())), preferred_element_type=F32)


LAG = 3
D_AT = [1,7,13,19,25,30,32,33,34]


class Links:
    def __init__(self, send_sems, recv_sems, partner):
        self.send_sems, self.recv_sems, self.partner = send_sems, recv_sems, partner
        self.n_send = self.n_recv = 0
        self.pending = []

    def slot(self):
        self.n_recv += 1
        return self.n_recv - 1

    def send(self, src, dst, device, slot, pred=None):
        copy = pltpu.make_async_remote_copy(
            src_ref=src,
            dst_ref=dst,
            send_sem=self.send_sems.at[self.n_send],
            recv_sem=self.recv_sems.at[slot],
            device_id=device,
            device_id_type=MESH,
        )
        self.n_send += 1
        self.pending.append((copy, pred))
        if pred is None:
            copy.start()
        else:
            pl.when(pred)(copy.start)

    def arrived(self, dst, slot, pred=None):
        copy = pltpu.make_async_remote_copy(
            src_ref=dst,
            dst_ref=dst,
            send_sem=self.send_sems.at[0],
            recv_sem=self.recv_sems.at[slot],
            device_id=self.partner,
            device_id_type=MESH,
        )
        if pred is None:
            copy.wait_recv()
        else:
            pl.when(pred)(copy.wait_recv)

    def drain(self):
        for copy, pred in self.pending:
            if pred is None:
                copy.wait_send()
            else:
                pl.when(pred)(copy.wait_send)
        self.pending = []


def together(*flows):
    flows = list(flows)
    while flows:
        for flow in list(flows):
            if next(flow, "end") == "end":
                flows.remove(flow)
        yield


def interleave(*flows):
    for _ in together(*flows):
        pass


def kernel(
    orb_hbm,
    proj_hbm,
    int_ref,
    exch_ref,
    back_ref,
    scal_ref,
    orb_ref,
    proj_ref,
    iv,
    pp,
    part,
    xs,
    xr,
    zs,
    zr,
    stage,
    full,
    hf,
    h16,
    hp,
    hh,
    acc,
    psend,
    prcv,
    ts,
    tr,
    tfull,
    dxs,
    dxr,
    dzs,
    dzr,
    ap,
    bk,
    bkr,
    sc,
    sr1,
    sr2,
    sr3,
    send_sems,
    recv_sems,
    int_sem,
):
    gx, gy = lax.axis_index("gx"), lax.axis_index("gy")
    z, x = gx // NX, gx % NX
    y, c = gy // NC, gy % NC
    rows = proj_ref.shape[0]
    npri = proj_ref.shape[1]
    nocc = orb_ref.shape[0]
    out_rows = rows // NX

    load = pltpu.make_async_copy(int_ref.at[0], iv, int_sem.at[0])
    load_proj = pltpu.make_async_copy(proj_hbm, proj_ref, int_sem.at[1])
    load_orb = pltpu.make_async_copy(orb_hbm, orb_ref, int_sem.at[2])

    def at(dz=0, dx=0, dy=0, dg=0):
        zz, xx = (z + dz) % NZ, (x + dx) % NX
        if dg:
            gg = (gy + dg) % NG
        else:
            gg = ((y + dy) % NY) * NC + c
        return (zz * NX + xx, gg)

    partner = (gx, y * NC + (1 - c))
    links = Links(send_sems, recv_sems, partner)

    barrier = pltpu.get_barrier_semaphore()
    peers = [at(dz=d) for d in range(1, NZ)] + [at(dx=d) for d in range(1, NX)]
    peers += [at(dg=d) for d in range(1, NG)]
    for peer in peers:
        pl.semaphore_signal(barrier, inc=1, device_id=peer, device_id_type=MESH)
    load_orb.start()
    load_proj.start()
    load.start()

    part[...] = jnp.zeros_like(part)
    load_orb.wait()
    load_proj.wait()
    share = dot(proj_ref[...], orb_ref[...], 1, 1)
    part[0, 0:rows, :] = share[:, 0:128]
    part[1, 0:rows, 0 : nocc - 128] = share[:, 128:nocc]
    pl.semaphore_wait(barrier, len(peers))

    def ring4(dim, part_of, on_arrival=None):
        me = {"x": x, "y": y}[dim]
        step = (lambda d: at(dx=d)) if dim == "x" else (lambda d: at(dy=d))
        left, right, far = (me + 3) % 4, (me + 1) % 4, (me + 2) % 4
        from_left, from_right, from_far = [[links.slot(), links.slot()] for _ in range(3)]

        def send(i, h, d, slots):
            links.send(part_of(i, h), part_of(i, h), step(d), slots[h])

        def arrived(i, h, slots):
            links.arrived(part_of(i, h), slots[h])

        def seen(i, h):
            if on_arrival:
                on_arrival(part_of, i, h)

        send(me, 0, 1, from_left)
        send(me, 1, 3, from_right)
        send(me, 1, 1, from_left)
        send(me, 0, 3, from_right)
        yield
        arrived(left, 0, from_left)
        send(left, 0, 1, from_far)
        arrived(right, 1, from_right)
        send(right, 1, 3, from_far)
        seen(left, 0)
        seen(right, 1)
        yield
        arrived(left, 1, from_left)
        arrived(right, 0, from_right)
        seen(left, 1)
        seen(right, 0)
        for h in range(2):
            arrived(far, h, from_far)
            seen(far, h)

    def direct4(dim, whole):
        me = {"x": x, "y": y}[dim]
        step = (lambda d: at(dx=d)) if dim == "x" else (lambda d: at(dy=d))
        slots = [links.slot() for _ in range(3)]
        for d in (2, 1, 3):
            links.send(whole(me), whole(me), step(d), slots[d - 1])
        yield
        for d in (1, 3, 2):
            links.arrived(whole((me + 4 - d) % 4), slots[d - 1])

    def reduce_xz(src_ref, xs, xr, zs, zr, piece, lanes):
        xs[lanes] = src_ref[lanes].astype(BF16)
        slots = [links.slot() for _ in range(1, NX)]
        for d in (2, 1, 3):
            to = (x + d) % NX
            links.send(xs.at[lanes, pl.ds(to * 192, 192)], xr.at[lanes, d - 1], at(dx=d), slots[d - 1])
        yield
        total = src_ref[lanes, pl.ds(x * 192, 192)]
        for d in (1, 3, 2):
            links.arrived(xr.at[lanes, d - 1], slots[d - 1])
            total = total + xr[lanes, d - 1].astype(F32)
        src_ref[lanes, pl.ds(x * 192, 192)] = total
        zs[lanes] = total.astype(BF16)
        slots = [links.slot() for _ in range(1, NZ)]
        for d in (4, 3, 5, 2, 6, 1, 7):
            to = (z + d) % NZ
            first = jnp.minimum(to, PIECES - 1) * 32
            links.send(zs.at[lanes, pl.ds(first, 32)], zr.at[lanes, d - 1], at(dz=d), slots[d - 1], to < PIECES)
        yield
        owner = z < PIECES
        for d in range(1, NZ):
            links.arrived(zr.at[lanes, d - 1], slots[d - 1], owner)

        own = jnp.minimum(z, PIECES - 1)

        @pl.when(owner)
        def _():
            total = src_ref[lanes, pl.ds(x * 192 + own * 32, 32)]
            for d in range(1, NZ):
                total = total + zr[lanes, d - 1].astype(F32)
            piece(x, own)[...] = total.astype(BF16)

        slots = [links.slot() for _ in range(1, NZ)]
        for d in (4, 3, 5, 2, 6, 1, 7):
            links.send(piece(x, own), piece(x, own), at(dz=d), slots[d - 1], owner)
        yield
        for d in range(1, NZ):
            src = (z + NZ - d) % NZ
            links.arrived(piece(x, jnp.minimum(src, PIECES - 1)), slots[d - 1], src < PIECES)

    def flow_admm(lanes):
        waits = []

        def to_partner(other):
            def go(part_of, i, h):
                slot = links.slot()
                links.send(part_of(i, h), part_of(i, h), partner, slot)
                waits.append((other, i, h, slot))

            return go

        yield from reduce_xz(part, xs, xr, zs, zr, lambda i, k: stage.at[lanes, y, c, i, pl.ds(k * 32, 32)], lanes)
        yield from together(
            direct4("x", lambda i: stage.at[lanes, y, c, i, 0:96]),
            direct4("y", lambda i: stage.at[lanes, i, c, x, 96:192]),
        )
        low = lambda i, h: stage.at[lanes, i, c, 2 * h : 2 * h + 2, 0:96]
        high = lambda i, h: stage.at[lanes, 2 * h : 2 * h + 2, c, i, 96:192]
        low_sent = to_partner(lambda i, h: stage.at[lanes, i, 1 - c, 2 * h : 2 * h + 2, 0:96])
        high_sent = to_partner(lambda i, h: stage.at[lanes, 2 * h : 2 * h + 2, 1 - c, i, 96:192])
        both = together(ring4("y", low, low_sent), ring4("x", high, high_sent))
        next(both)
        for h in range(2):
            low_sent(low, y, h)
            high_sent(high, x, h)
        yield
        yield from both
        for other, i, h, slot in waits:
            links.arrived(other(i, h), slot)

    def housekeeping():
        pp[...] = jnp.zeros_like(pp)
        pp[0:rows, 0:npri] = proj_ref[...]
        hf[...] = jnp.zeros_like(hf)
        hp[...] = jnp.zeros_like(hp)
        yield

    flows = [flow_admm(0), flow_admm(1)]
    interleave(*flows, housekeeping())
    for a in range(NY):
        for b in range(NC):
            for k in range(NX):
                n = min(192, rows - 192 * k)
                r0 = rows * (a * NC + b) + 192 * k
                full[r0 : r0 + n, 0:128] = stage[0, a, b, k, 0:n, :]
                full[r0 : r0 + n, 128:256] = stage[1, a, b, k, 0:n, :]

    load.wait()
    for r0 in range(0, rows, 256):
        n = min(256, rows - r0)
        hf[r0 : r0 + n, :] = dot(iv[r0 : r0 + n, :], full[...], 1, 0)
    h16[...] = hf[...].astype(BF16)
    hr = h16[...].astype(F32)
    trace = jnp.sum(hr * hr)
    for k in range(NX):
        hp[192 * k : 192 * k + out_rows, :] = hf[out_rows * k : out_rows * (k + 1), :]
    ht = jnp.transpose(hp[...])[0:208, :].astype(BF16)
    for j in range(6):
        hh[0, 0, j] = ht[:, 128 * j : 128 * j + 128]

    ys, cs = z // NC, z % NC
    dy = (y + NY - ys) % NY
    on = c == cs
    is_src = on & (dy == 0)
    lhs_at = jnp.where(is_src, 0, 1)
    up, down, yup, ydown = at(dz=1), at(dz=NZ - 1), at(dy=1), at(dy=NY - 1)

    def piece_of(which, s, j):
        return hh.at[which, s, j]

    def accumulate_half(slots, m, first=False):
        lhs = jnp.concatenate(
            [jnp.concatenate([hh[lhs_at, s, 3 * m + i] for i in range(3)], 1) for s in slots], 0
        )
        rhs = jnp.concatenate([jnp.concatenate([hh[0, s, j] for j in range(6)], 1) for s in slots], 0)
        value = dot(lhs, rhs, 0, 0)
        here = pl.ds(pl.multiple_of(m * 384, 384), 384)
        if first:
            acc[here, :] = value
        else:
            acc[here, :] += value

    def accumulate(*slots, first=False):
        @pl.loop(0, 2)
        def _(m):
            accumulate_half(slots, m, first)

    def flow_exchange():
        col_slots = {(s, j): links.slot() for s in range(1, NZ) for j in range(6)}
        row_slots = {(s, j): links.slot() for s in range(NZ) for j in range(6)}
        pairs = {e - 2: [(0, e), (0, 5 - e)] for e in range(3)}
        for k in (1, 2, 3):
            for j in range(6):
                pairs[6 * k - 5 + j] = [(k, j), (8 - k, 5 - j)]
        for j in range(3):
            pairs[19 + j] = [(4, j), (4, 5 - j)]

        def pass_on(s, j):
            if s in (0, 1, 2) or (s == 3 and j < 3):
                links.send(piece_of(0, s, j), piece_of(0, s + 1, j), up, col_slots[s + 1, j])
            if s in (0, 7, 6) or (s == 5 and j >= 3):
                t = (s - 1) % 8
                links.send(piece_of(0, s, j), piece_of(0, t, j), down, col_slots[t, j])

        def spread(s, j):
            src, dst = piece_of(0, s, j), piece_of(1, s, j)
            links.send(src, dst, yup if j < 3 else ydown, row_slots[s, j], is_src)
            links.send(src, dst, partner, row_slots[s, j], is_src)

        def relay(s, j, h):
            blk = piece_of(1, s, j)
            here = on & (dy == (h if j < 3 else 4 - h))
            links.arrived(blk, row_slots[s, j], here)
            if h < 3:
                links.send(blk, blk, yup if j < 3 else ydown, row_slots[s, j], here)
            links.send(blk, blk, partner, row_slots[s, j], here)

        def rows_here(*slots):
            for s in slots:
                for j in range(6):
                    links.arrived(piece_of(1, s, j), row_slots[s, j], jnp.logical_not(on))

        for j in range(6):
            pass_on(0, [0, 5, 1, 4, 2, 3][j])
        yield
        for j in range(6):
            spread(0, [0, 5, 1, 4, 2, 3][j])
        yield
        last = 21 + 3 * LAG
        for e in range(0, last + 1):
            if 1 <= e <= 21:
                for s, j in pairs[e]:
                    links.arrived(piece_of(0, s, j), col_slots[s, j])
                    pass_on(s, j)
                    spread(s, j)
            for h in (1, 2, 3):
                for s, j in pairs.get(e - LAG * h, ()):
                    relay(s, j, h)
            q = e - 3 * LAG - 1
            if q in (6, 12, 18):
                k = q // 6
                slots = (0, 1, 7) if k == 1 else (k, 8 - k)
                rows_here(*slots)
                accumulate(*slots, first=k == 1)
            yield
        rows_here(4)
        slots = [links.slot() for _ in range(6)]
        left, right, far = (x + 3) % NX, (x + 1) % NX, (x + 2) % NX
        to_right, to_left = at(dx=1), at(dx=3)
        def mine(i, h):
            return acc[pl.ds(i * 192, 192), 384 * h : 384 * h + 384]

        far_half = 1 - x // 2
        accumulate_half((4,), far_half)
        psend[0] = mine(far, 0).astype(BF16)
        links.send(psend.at[0], prcv.at[0], to_right, slots[0])
        psend[1] = mine(far, 1).astype(BF16)
        links.send(psend.at[1], prcv.at[1], to_left, slots[1])
        accumulate_half((4,), 1 - far_half)
        psend[2] = mine(right, 1).astype(BF16)
        links.send(psend.at[2], prcv.at[2], to_right, slots[2])
        psend[3] = mine(left, 0).astype(BF16)
        links.send(psend.at[3], prcv.at[3], to_left, slots[3])
        yield
        links.arrived(prcv.at[0], slots[0])
        psend[4] = (mine(right, 0) + prcv[0].astype(F32)).astype(BF16)
        links.send(psend.at[4], prcv.at[4], to_right, slots[4])
        links.arrived(prcv.at[1], slots[1])
        psend[5] = (mine(left, 1) + prcv[1].astype(F32)).astype(BF16)
        links.send(psend.at[5], prcv.at[5], to_left, slots[5])
        yield
        for j in (2, 3, 4, 5):
            links.arrived(prcv.at[j], slots[j])
        first = mine(x, 0) + prcv[3].astype(F32) + prcv[4].astype(F32)
        second = mine(x, 1) + prcv[2].astype(F32) + prcv[5].astype(F32)
        total = jnp.concatenate([first, second], 1)
        lane = lax.broadcasted_iota(jnp.int32, total.shape, 1)
        out = total
        for k in range(1, NX):
            moved = pltpu.roll(total, total.shape[1] - 4 * k, 1)
            out = jnp.where(lane >= out_rows * k, moved, out)
        exch_ref[...] = out[0:out_rows, 0:rows]

    def flow_applied():
        own = jnp.concatenate([stage[i, y, c].reshape(4 * 192, 128) for i in range(2)], 1)
        tt = dot(own, h16[...], 0, 0).astype(BF16)
        share = nocc // NG
        r = lax.broadcasted_iota(jnp.int32, (256, 256), 0)
        j = lax.broadcasted_iota(jnp.int32, (256, 256), 1)
        pick = ((r % 32 < share) & (j == share * (r // 32) + r % 32)).astype(F32).astype(BF16)
        ts[...] = dot(pick, tt, 1, 0).astype(BF16)
        slots = [links.slot() for _ in range(1, NG)]
        for d in range(1, NG):
            to = (gy + d) % NG
            links.send(ts.at[pl.ds(to * 32, 32), :], tr.at[d - 1], at(dg=d), slots[d - 1])
        yield
        total = ts[pl.ds(gy * 32, 32), :].astype(F32)
        for d in range(1, NG):
            links.arrived(tr.at[d - 1], slots[d - 1])
            total = total + tr[d - 1].astype(F32)
        energy = jnp.sum(total * total)
        tfull[pl.ds(gy * 32, 32), :] = total.astype(BF16)
        slots = [links.slot() for _ in range(1, NG)]
        s1 = [links.slot() for _ in range(1, NG)]
        mine = tfull.at[pl.ds(gy * 32, 32), :]
        sc[0] = jnp.where(lax.broadcasted_iota(jnp.int32, (8, 128), 0) == 0, trace, energy)
        for d in range(1, NG):
            links.send(mine, mine, at(dg=d), slots[d - 1])
            links.send(sc.at[0], sr1.at[d - 1], at(dg=d), s1[d - 1])
        yield
        for d in range(1, NG):
            src = (gy + NG - d) % NG
            links.arrived(tfull.at[pl.ds(src * 32, 32), :], slots[d - 1])
        applied = dot(h16[...], tfull[...], 1, 1)
        part[0] = applied[:, 0:128]
        part[1] = applied[:, 128:256]
        total = sc[0]
        for d in range(1, NG):
            links.arrived(sr1.at[d - 1], s1[d - 1])
            total = total + sr1[d - 1]
        sc[1] = total
        s2 = [links.slot() for _ in range(1, NX)]
        for d in range(1, NX):
            links.send(sc.at[1], sr2.at[d - 1], at(dx=d), s2[d - 1])
        for _ in reduce_xz(part, dxs, dxr, dzs, dzr, lambda i, k: ap.at[:, i, pl.ds(k * 32, 32)], slice(0, 2)):
            yield
        total = sc[1]
        for d in range(1, NX):
            links.arrived(sr2.at[d - 1], s2[d - 1])
            total = total + sr2[d - 1]
        sc[2] = total
        s3 = [links.slot() for _ in range(1, NZ)]
        for d in range(1, NZ):
            links.send(sc.at[2], sr3.at[d - 1], at(dz=d), s3[d - 1])
        for _ in ring4("x", lambda i, h: ap.at[h, i]):
            yield
        whole = jnp.concatenate([ap[i].reshape(4 * 192, 128) for i in range(2)], 1)
        bt = dot(whole, pp[...], 0, 0)
        bk[...] = bt.astype(BF16)
        slots = [links.slot() for _ in range(1, NG)]
        for d in range(1, NG):
            to = (gy + d) % NG
            links.send(bk.at[pl.ds(to * 32, 32), :], bkr.at[d - 1], at(dg=d), slots[d - 1])
        yield
        total = bk[pl.ds(gy * 32, 32), :].astype(F32)
        for d in range(1, NG):
            links.arrived(bkr.at[d - 1], slots[d - 1])
            total = total + bkr[d - 1].astype(F32)
        back_ref[...] = total
        total = sc[2]
        for d in range(1, NZ):
            links.arrived(sr3.at[d - 1], s3[d - 1])
            total = total + sr3[d - 1]
        scal_ref[...] = total

    exchange, applied = flow_exchange(), flow_applied()
    for step, _ in enumerate(exchange):
        for _ in range(D_AT.count(step)):
            next(applied, None)
    for _ in applied:
        pass
    links.drain()


N_SEMS = 720


def finish(total_adm, nocc, exch_ref, back_ref, scal_ref, exch_out, back_out, energy_out, trace_out):
    exch_out[...] = exch_ref[...]
    back_out[...] = back_ref[0 : back_out.shape[0], 0 : back_out.shape[1]]
    trace_out[...] = scal_ref[0:1, 0:1] / total_adm
    energy_out[...] = -0.5 * scal_ref[1:2, 0:1] / (total_adm * nocc)


def on_device(orbitals, projector, integrals):
    rows, npri = projector.shape
    total_adm = integrals.shape[2]
    nocc = orbitals.shape[1]
    out_rows = rows // NX
    vmem = pl.BlockSpec(memory_space=pltpu.VMEM)
    scratch = [
        pltpu.VMEM((nocc, npri), BF16),
        pltpu.VMEM((rows, npri), BF16),
        pltpu.VMEM((rows, total_adm), BF16),
        pltpu.VMEM((768, 640), BF16),
        pltpu.VMEM((2, 768, 128), F32),
        pltpu.VMEM((2, 768, 128), BF16),
        pltpu.VMEM((2, 3, 192, 128), BF16),
        pltpu.VMEM((2, 192, 128), BF16),
        pltpu.VMEM((2, 7, 32, 128), BF16),
        pltpu.VMEM((2, NY, NC, NX, 192, 128), BF16),
        pltpu.VMEM((total_adm, 256), BF16),
        pltpu.VMEM((768, 256), F32),
        pltpu.VMEM((768, 256), BF16),
        pltpu.VMEM((768, 256), F32),
        pltpu.VMEM((2, NZ, 6, 208, 128), BF16),
        pltpu.VMEM((768, 768), F32),
        pltpu.VMEM((6, 192, 384), BF16),
        pltpu.VMEM((6, 192, 384), BF16),
        pltpu.VMEM((256, 256), BF16),
        pltpu.VMEM((7, 32, 256), BF16),
        pltpu.VMEM((256, 256), BF16),
        pltpu.VMEM((2, 768, 128), BF16),
        pltpu.VMEM((2, 3, 192, 128), BF16),
        pltpu.VMEM((2, 192, 128), BF16),
        pltpu.VMEM((2, 7, 32, 128), BF16),
        pltpu.VMEM((2, NX, 192, 128), BF16),
        pltpu.VMEM((256, 640), BF16),
        pltpu.VMEM((7, 32, 640), BF16),
        pltpu.VMEM((3, 8, 128), F32),
        pltpu.VMEM((7, 8, 128), F32),
        pltpu.VMEM((3, 8, 128), F32),
        pltpu.VMEM((7, 8, 128), F32),
        pltpu.SemaphoreType.DMA((N_SEMS,)),
        pltpu.SemaphoreType.DMA((N_SEMS,)),
        pltpu.SemaphoreType.DMA((3,)),
    ]
    exchange, back, scal = pl.pallas_call(
        kernel,
        out_shape=(
            jax.ShapeDtypeStruct((out_rows, rows), F32),
            jax.ShapeDtypeStruct((32, 640), F32),
            jax.ShapeDtypeStruct((8, 128), F32),
        ),
        in_specs=[pl.BlockSpec(memory_space=pl.ANY)] * 3,
        out_specs=(vmem, vmem, vmem),
        scratch_shapes=scratch,
        compiler_params=pltpu.CompilerParams(
            collective_id=0, has_side_effects=True, vmem_limit_bytes=56 * 1024 * 1024
        ),
        name="admm_exchange",
    )(orbitals.T, projector, integrals)
    exchange, back, energy_mean, trace_mean = pl.pallas_call(
        functools.partial(finish, total_adm, nocc),
        out_shape=(
            jax.ShapeDtypeStruct((out_rows, rows), F32),
            jax.ShapeDtypeStruct((nocc // NG, npri), F32),
            jax.ShapeDtypeStruct((1, 1), F32),
            jax.ShapeDtypeStruct((1, 1), F32),
        ),
        in_specs=[vmem] * 3,
        out_specs=(vmem,) * 4,
        name="finish",
    )(exchange, back, scal)
    return exchange, back.T, energy_mean.reshape(()), trace_mean.reshape(())


def solution(mesh):
    return jax.shard_map(
        on_device,
        mesh=mesh,
        in_specs=(P("gx", None), P("gy", "gx"), P("gx", "gy", None)),
        out_specs=(P("gx", "gy"), P("gx", "gy"), P(), P()),
        check_vma=False,
    )
```

```python
import functools

import jax
import jax.numpy as jnp
from jax import lax
from jax.experimental import pallas as pl
from jax.experimental.pallas import tpu as pltpu
from jax.sharding import PartitionSpec as P

MESH = pl.DeviceIdType.MESH
F32, BF16 = jnp.float32, jnp.bfloat16
NZ, NX, NY, NC = 8, 4, 4, 2
NG = NY * NC
PIECES = 6


def dot(a, b, ca, cb):
    return lax.dot_general(a, b, (((ca,), (cb,)), ((), ())), preferred_element_type=F32)


LAG = 3
D_AT = [1,7,13,19,25,30,33,34]


class Links:
    def __init__(self, send_sems, recv_sems, partner):
        self.send_sems, self.recv_sems, self.partner = send_sems, recv_sems, partner
        self.n_send = self.n_recv = 0
        self.pending = []

    def slot(self):
        self.n_recv += 1
        return self.n_recv - 1

    def send(self, src, dst, device, slot, pred=None):
        copy = pltpu.make_async_remote_copy(
            src_ref=src,
            dst_ref=dst,
            send_sem=self.send_sems.at[self.n_send],
            recv_sem=self.recv_sems.at[slot],
            device_id=device,
            device_id_type=MESH,
        )
        self.n_send += 1
        self.pending.append((copy, pred))
        if pred is None:
            copy.start()
        else:
            pl.when(pred)(copy.start)

    def arrived(self, dst, slot, pred=None):
        copy = pltpu.make_async_remote_copy(
            src_ref=dst,
            dst_ref=dst,
            send_sem=self.send_sems.at[0],
            recv_sem=self.recv_sems.at[slot],
            device_id=self.partner,
            device_id_type=MESH,
        )
        if pred is None:
            copy.wait_recv()
        else:
            pl.when(pred)(copy.wait_recv)

    def drain(self):
        for copy, pred in self.pending:
            if pred is None:
                copy.wait_send()
            else:
                pl.when(pred)(copy.wait_send)
        self.pending = []


def together(*flows):
    flows = list(flows)
    while flows:
        for flow in list(flows):
            if next(flow, "end") == "end":
                flows.remove(flow)
        yield


def interleave(*flows):
    for _ in together(*flows):
        pass


def kernel(
    orb_hbm,
    proj_hbm,
    int_ref,
    exch_ref,
    back_ref,
    scal_ref,
    orb_ref,
    proj_ref,
    iv,
    pp,
    part,
    xs,
    xr,
    zs,
    zr,
    stage,
    full,
    hf,
    h16,
    hp,
    hh,
    acc,
    psend,
    prcv,
    ts,
    tr,
    tfull,
    dxs,
    dxr,
    dzs,
    dzr,
    ap,
    bk,
    bkr,
    sc,
    sr1,
    sr2,
    sr3,
    send_sems,
    recv_sems,
    int_sem,
):
    gx, gy = lax.axis_index("gx"), lax.axis_index("gy")
    z, x = gx // NX, gx % NX
    y, c = gy // NC, gy % NC
    rows = proj_ref.shape[0]
    npri = proj_ref.shape[1]
    nocc = orb_ref.shape[0]
    out_rows = rows // NX

    load = pltpu.make_async_copy(int_ref.at[0], iv, int_sem.at[0])
    load_proj = pltpu.make_async_copy(proj_hbm, proj_ref, int_sem.at[1])
    load_orb = pltpu.make_async_copy(orb_hbm, orb_ref, int_sem.at[2])

    def at(dz=0, dx=0, dy=0, dg=0):
        zz, xx = (z + dz) % NZ, (x + dx) % NX
        if dg:
            gg = (gy + dg) % NG
        else:
            gg = ((y + dy) % NY) * NC + c
        return (zz * NX + xx, gg)

    partner = (gx, y * NC + (1 - c))
    links = Links(send_sems, recv_sems, partner)

    barrier = pltpu.get_barrier_semaphore()
    peers = [at(dz=d) for d in range(1, NZ)] + [at(dx=d) for d in range(1, NX)]
    peers += [at(dg=d) for d in range(1, NG)]
    for peer in peers:
        pl.semaphore_signal(barrier, inc=1, device_id=peer, device_id_type=MESH)
    load_orb.start()
    load_proj.start()
    load.start()

    part[...] = jnp.zeros_like(part)
    load_orb.wait()
    load_proj.wait()
    share = dot(proj_ref[...], orb_ref[...], 1, 1)
    part[0, 0:rows, :] = share[:, 0:128]
    part[1, 0:rows, 0 : nocc - 128] = share[:, 128:nocc]
    pl.semaphore_wait(barrier, len(peers))

    def ring4(dim, part_of, on_arrival=None):
        me = {"x": x, "y": y}[dim]
        step = (lambda d: at(dx=d)) if dim == "x" else (lambda d: at(dy=d))
        left, right, far = (me + 3) % 4, (me + 1) % 4, (me + 2) % 4
        from_left, from_right, from_far = [[links.slot(), links.slot()] for _ in range(3)]

        def send(i, h, d, slots):
            links.send(part_of(i, h), part_of(i, h), step(d), slots[h])

        def arrived(i, h, slots):
            links.arrived(part_of(i, h), slots[h])

        def seen(i, h):
            if on_arrival:
                on_arrival(part_of, i, h)

        send(me, 0, 1, from_left)
        send(me, 1, 3, from_right)
        send(me, 1, 1, from_left)
        send(me, 0, 3, from_right)
        yield
        arrived(left, 0, from_left)
        send(left, 0, 1, from_far)
        arrived(right, 1, from_right)
        send(right, 1, 3, from_far)
        seen(left, 0)
        seen(right, 1)
        yield
        arrived(left, 1, from_left)
        arrived(right, 0, from_right)
        seen(left, 1)
        seen(right, 0)
        for h in range(2):
            arrived(far, h, from_far)
            seen(far, h)

    def direct4(dim, whole):
        me = {"x": x, "y": y}[dim]
        step = (lambda d: at(dx=d)) if dim == "x" else (lambda d: at(dy=d))
        slots = [links.slot() for _ in range(3)]
        for d in (2, 1, 3):
            links.send(whole(me), whole(me), step(d), slots[d - 1])
        yield
        for d in (1, 3, 2):
            links.arrived(whole((me + 4 - d) % 4), slots[d - 1])

    def reduce_xz(src_ref, xs, xr, zs, zr, piece, lanes):
        xs[lanes] = src_ref[lanes].astype(BF16)
        slots = [links.slot() for _ in range(1, NX)]
        for d in (2, 1, 3):
            to = (x + d) % NX
            links.send(xs.at[lanes, pl.ds(to * 192, 192)], xr.at[lanes, d - 1], at(dx=d), slots[d - 1])
        yield
        total = src_ref[lanes, pl.ds(x * 192, 192)]
        for d in (1, 3, 2):
            links.arrived(xr.at[lanes, d - 1], slots[d - 1])
            total = total + xr[lanes, d - 1].astype(F32)
        src_ref[lanes, pl.ds(x * 192, 192)] = total
        zs[lanes] = total.astype(BF16)
        slots = [links.slot() for _ in range(1, NZ)]
        for d in (4, 3, 5, 2, 6, 1, 7):
            to = (z + d) % NZ
            first = jnp.minimum(to, PIECES - 1) * 32
            links.send(zs.at[lanes, pl.ds(first, 32)], zr.at[lanes, d - 1], at(dz=d), slots[d - 1], to < PIECES)
        yield
        owner = z < PIECES
        for d in range(1, NZ):
            links.arrived(zr.at[lanes, d - 1], slots[d - 1], owner)

        own = jnp.minimum(z, PIECES - 1)

        @pl.when(owner)
        def _():
            total = src_ref[lanes, pl.ds(x * 192 + own * 32, 32)]
            for d in range(1, NZ):
                total = total + zr[lanes, d - 1].astype(F32)
            piece(x, own)[...] = total.astype(BF16)

        slots = [links.slot() for _ in range(1, NZ)]
        for d in (4, 3, 5, 2, 6, 1, 7):
            links.send(piece(x, own), piece(x, own), at(dz=d), slots[d - 1], owner)
        yield
        for d in range(1, NZ):
            src = (z + NZ - d) % NZ
            links.arrived(piece(x, jnp.minimum(src, PIECES - 1)), slots[d - 1], src < PIECES)

    def flow_admm(lanes):
        waits = []

        def to_partner(other):
            def go(part_of, i, h):
                slot = links.slot()
                links.send(part_of(i, h), part_of(i, h), partner, slot)
                waits.append((other, i, h, slot))

            return go

        yield from reduce_xz(part, xs, xr, zs, zr, lambda i, k: stage.at[lanes, y, c, i, pl.ds(k * 32, 32)], lanes)
        yield from together(
            direct4("x", lambda i: stage.at[lanes, y, c, i, 0:96]),
            direct4("y", lambda i: stage.at[lanes, i, c, x, 96:192]),
        )
        low = lambda i, h: stage.at[lanes, i, c, 2 * h : 2 * h + 2, 0:96]
        high = lambda i, h: stage.at[lanes, 2 * h : 2 * h + 2, c, i, 96:192]
        low_sent = to_partner(lambda i, h: stage.at[lanes, i, 1 - c, 2 * h : 2 * h + 2, 0:96])
        high_sent = to_partner(lambda i, h: stage.at[lanes, 2 * h : 2 * h + 2, 1 - c, i, 96:192])
        both = together(ring4("y", low, low_sent), ring4("x", high, high_sent))
        next(both)
        for h in range(2):
            low_sent(low, y, h)
            high_sent(high, x, h)
        yield
        yield from both
        for other, i, h, slot in waits:
            links.arrived(other(i, h), slot)

    def housekeeping():
        pp[...] = jnp.zeros_like(pp)
        pp[0:rows, 0:npri] = proj_ref[...]
        hf[...] = jnp.zeros_like(hf)
        hp[...] = jnp.zeros_like(hp)
        yield

    flows = [flow_admm(0), flow_admm(1)]
    interleave(*flows, housekeeping())
    for a in range(NY):
        for b in range(NC):
            for k in range(NX):
                n = min(192, rows - 192 * k)
                r0 = rows * (a * NC + b) + 192 * k
                full[r0 : r0 + n, 0:128] = stage[0, a, b, k, 0:n, :]
                full[r0 : r0 + n, 128:256] = stage[1, a, b, k, 0:n, :]

    load.wait()
    for r0 in range(0, rows, 256):
        n = min(256, rows - r0)
        hf[r0 : r0 + n, :] = dot(iv[r0 : r0 + n, :], full[...], 1, 0)
    h16[...] = hf[...].astype(BF16)
    hr = h16[...].astype(F32)
    trace = jnp.sum(hr * hr)
    for k in range(NX):
        hp[192 * k : 192 * k + out_rows, :] = hf[out_rows * k : out_rows * (k + 1), :]
    ht = jnp.transpose(hp[...])[0:208, :].astype(BF16)
    for j in range(6):
        hh[0, 0, j] = ht[:, 128 * j : 128 * j + 128]

    ys, cs = z // NC, z % NC
    dy = (y + NY - ys) % NY
    on = c == cs
    is_src = on & (dy == 0)
    lhs_at = jnp.where(is_src, 0, 1)
    up, down, yup, ydown = at(dz=1), at(dz=NZ - 1), at(dy=1), at(dy=NY - 1)

    def piece_of(which, s, j):
        return hh.at[which, s, j]

    def accumulate_half(slots, m, first=False):
        lhs = jnp.concatenate(
            [jnp.concatenate([hh[lhs_at, s, 3 * m + i] for i in range(3)], 1) for s in slots], 0
        )
        rhs = jnp.concatenate([jnp.concatenate([hh[0, s, j] for j in range(6)], 1) for s in slots], 0)
        value = dot(lhs, rhs, 0, 0)
        here = pl.ds(pl.multiple_of(m * 384, 384), 384)
        if first:
            acc[here, :] = value
        else:
            acc[here, :] += value

    def accumulate(*slots, first=False):
        @pl.loop(0, 2)
        def _(m):
            accumulate_half(slots, m, first)

    def flow_exchange():
        col_slots = {(s, j): links.slot() for s in range(1, NZ) for j in range(6)}
        row_slots = {(s, j): links.slot() for s in range(NZ) for j in range(6)}
        pairs = {e - 2: [(0, e), (0, 5 - e)] for e in range(3)}
        for k in (1, 2, 3):
            for j in range(6):
                pairs[6 * k - 5 + j] = [(k, j), (8 - k, 5 - j)]
        for j in range(3):
            pairs[19 + j] = [(4, j), (4, 5 - j)]

        def pass_on(s, j):
            if s in (0, 1, 2) or (s == 3 and j < 3):
                links.send(piece_of(0, s, j), piece_of(0, s + 1, j), up, col_slots[s + 1, j])
            if s in (0, 7, 6) or (s == 5 and j >= 3):
                t = (s - 1) % 8
                links.send(piece_of(0, s, j), piece_of(0, t, j), down, col_slots[t, j])

        def goes_up(s, j):
            return j < 3

        def spread(s, j):
            src, dst = piece_of(0, s, j), piece_of(1, s, j)
            if s == 4 or goes_up(s, j):
                links.send(src, dst, yup, row_slots[s, j], is_src)
            if s == 4 or not goes_up(s, j):
                links.send(src, dst, ydown, row_slots[s, j], is_src)
            links.send(src, dst, partner, row_slots[s, j], is_src)

        def relay(s, j, h):
            blk = piece_of(1, s, j)
            side = h if goes_up(s, j) else 4 - h
            here = on & (dy == side)
            if s == 4:
                if h == 3:
                    return
                if h == 1:
                    here = on & ((dy == 1) | (dy == 3))
            links.arrived(blk, row_slots[s, j], here)
            if h < (2 if s == 4 else 3):
                links.send(blk, blk, yup if goes_up(s, j) else ydown, row_slots[s, j], on & (dy == side))
            links.send(blk, blk, partner, row_slots[s, j], here)

        def rows_here(*slots):
            for s in slots:
                for j in range(6):
                    links.arrived(piece_of(1, s, j), row_slots[s, j], jnp.logical_not(on))

        for j in range(6):
            pass_on(0, [0, 5, 1, 4, 2, 3][j])
        yield
        for j in range(6):
            spread(0, [0, 5, 1, 4, 2, 3][j])
        yield
        last = 21 + 3 * LAG
        for e in range(0, last + 1):
            if 1 <= e <= 21:
                for s, j in pairs[e]:
                    links.arrived(piece_of(0, s, j), col_slots[s, j])
                    pass_on(s, j)
                    spread(s, j)
            for h in (1, 2, 3):
                for s, j in pairs.get(e - LAG * h, ()):
                    relay(s, j, h)
            q = e - 3 * LAG - 1
            if q in (6, 12, 18):
                k = q // 6
                slots = (0, 1, 7) if k == 1 else (k, 8 - k)
                rows_here(*slots)
                accumulate(*slots, first=k == 1)
            yield
        rows_here(4)
        slots = [links.slot() for _ in range(6)]
        left, right, far = (x + 3) % NX, (x + 1) % NX, (x + 2) % NX
        to_right, to_left = at(dx=1), at(dx=3)
        def mine(i, h):
            return acc[pl.ds(i * 192, 192), 384 * h : 384 * h + 384]

        far_half = 1 - x // 2
        accumulate_half((4,), far_half)
        psend[0] = mine(far, 0).astype(BF16)
        links.send(psend.at[0], prcv.at[0], to_right, slots[0])
        psend[1] = mine(far, 1).astype(BF16)
        links.send(psend.at[1], prcv.at[1], to_left, slots[1])
        accumulate_half((4,), 1 - far_half)
        psend[2] = mine(right, 1).astype(BF16)
        links.send(psend.at[2], prcv.at[2], to_right, slots[2])
        psend[3] = mine(left, 0).astype(BF16)
        links.send(psend.at[3], prcv.at[3], to_left, slots[3])
        yield
        links.arrived(prcv.at[0], slots[0])
        psend[4] = (mine(right, 0) + prcv[0].astype(F32)).astype(BF16)
        links.send(psend.at[4], prcv.at[4], to_right, slots[4])
        links.arrived(prcv.at[1], slots[1])
        psend[5] = (mine(left, 1) + prcv[1].astype(F32)).astype(BF16)
        links.send(psend.at[5], prcv.at[5], to_left, slots[5])
        yield
        for j in (2, 3, 4, 5):
            links.arrived(prcv.at[j], slots[j])
        first = mine(x, 0) + prcv[3].astype(F32) + prcv[4].astype(F32)
        second = mine(x, 1) + prcv[2].astype(F32) + prcv[5].astype(F32)
        total = jnp.concatenate([first, second], 1)
        lane = lax.broadcasted_iota(jnp.int32, total.shape, 1)
        out = total
        for k in range(1, NX):
            moved = pltpu.roll(total, total.shape[1] - 4 * k, 1)
            out = jnp.where(lane >= out_rows * k, moved, out)
        exch_ref[...] = out[0:out_rows, 0:rows]

    def flow_applied():
        own = jnp.concatenate([stage[i, y, c].reshape(4 * 192, 128) for i in range(2)], 1)
        tt = dot(own, h16[...], 0, 0).astype(BF16)
        share = nocc // NG
        r = lax.broadcasted_iota(jnp.int32, (256, 256), 0)
        j = lax.broadcasted_iota(jnp.int32, (256, 256), 1)
        pick = ((r % 32 < share) & (j == share * (r // 32) + r % 32)).astype(F32).astype(BF16)
        ts[...] = dot(pick, tt, 1, 0).astype(BF16)
        slots = [links.slot() for _ in range(1, NG)]
        for d in range(1, NG):
            to = (gy + d) % NG
            links.send(ts.at[pl.ds(to * 32, 32), :], tr.at[d - 1], at(dg=d), slots[d - 1])
        yield
        total = ts[pl.ds(gy * 32, 32), :].astype(F32)
        for d in range(1, NG):
            links.arrived(tr.at[d - 1], slots[d - 1])
            total = total + tr[d - 1].astype(F32)
        energy = jnp.sum(total * total)
        tfull[pl.ds(gy * 32, 32), :] = total.astype(BF16)
        slots = [links.slot() for _ in range(1, NG)]
        s1 = [links.slot() for _ in range(1, NG)]
        mine = tfull.at[pl.ds(gy * 32, 32), :]
        sc[0] = jnp.where(lax.broadcasted_iota(jnp.int32, (8, 128), 0) == 0, trace, energy)
        for d in range(1, NG):
            links.send(mine, mine, at(dg=d), slots[d - 1])
            links.send(sc.at[0], sr1.at[d - 1], at(dg=d), s1[d - 1])
        yield
        for d in range(1, NG):
            src = (gy + NG - d) % NG
            links.arrived(tfull.at[pl.ds(src * 32, 32), :], slots[d - 1])
        applied = dot(h16[...], tfull[...], 1, 1)
        part[0] = applied[:, 0:128]
        part[1] = applied[:, 128:256]
        total = sc[0]
        for d in range(1, NG):
            links.arrived(sr1.at[d - 1], s1[d - 1])
            total = total + sr1[d - 1]
        sc[1] = total
        s2 = [links.slot() for _ in range(1, NX)]
        for d in range(1, NX):
            links.send(sc.at[1], sr2.at[d - 1], at(dx=d), s2[d - 1])
        for _ in reduce_xz(part, dxs, dxr, dzs, dzr, lambda i, k: ap.at[:, i, pl.ds(k * 32, 32)], slice(0, 2)):
            yield
        total = sc[1]
        for d in range(1, NX):
            links.arrived(sr2.at[d - 1], s2[d - 1])
            total = total + sr2[d - 1]
        sc[2] = total
        s3 = [links.slot() for _ in range(1, NZ)]
        for d in range(1, NZ):
            links.send(sc.at[2], sr3.at[d - 1], at(dz=d), s3[d - 1])
        for _ in direct4("x", lambda i: ap.at[:, i]):
            yield
        whole = jnp.concatenate([ap[i].reshape(4 * 192, 128) for i in range(2)], 1)
        bt = dot(whole, pp[...], 0, 0)
        bk[...] = bt.astype(BF16)
        slots = [links.slot() for _ in range(1, NG)]
        for d in range(1, NG):
            to = (gy + d) % NG
            links.send(bk.at[pl.ds(to * 32, 32), :], bkr.at[d - 1], at(dg=d), slots[d - 1])
        yield
        total = bk[pl.ds(gy * 32, 32), :].astype(F32)
        for d in range(1, NG):
            links.arrived(bkr.at[d - 1], slots[d - 1])
            total = total + bkr[d - 1].astype(F32)
        back_ref[...] = total
        total = sc[2]
        for d in range(1, NZ):
            links.arrived(sr3.at[d - 1], s3[d - 1])
            total = total + sr3[d - 1]
        scal_ref[...] = total

    exchange, applied = flow_exchange(), flow_applied()
    for step, _ in enumerate(exchange):
        for _ in range(D_AT.count(step)):
            next(applied, None)
    for _ in applied:
        pass
    links.drain()


N_SEMS = 720


def finish(total_adm, nocc, exch_ref, back_ref, scal_ref, exch_out, back_out, energy_out, trace_out):
    exch_out[...] = exch_ref[...]
    back_out[...] = back_ref[0 : back_out.shape[0], 0 : back_out.shape[1]]
    trace_out[...] = scal_ref[0:1, 0:1] / total_adm
    energy_out[...] = -0.5 * scal_ref[1:2, 0:1] / (total_adm * nocc)


def on_device(orbitals, projector, integrals):
    rows, npri = projector.shape
    total_adm = integrals.shape[2]
    nocc = orbitals.shape[1]
    out_rows = rows // NX
    vmem = pl.BlockSpec(memory_space=pltpu.VMEM)
    scratch = [
        pltpu.VMEM((nocc, npri), BF16),
        pltpu.VMEM((rows, npri), BF16),
        pltpu.VMEM((rows, total_adm), BF16),
        pltpu.VMEM((768, 640), BF16),
        pltpu.VMEM((2, 768, 128), F32),
        pltpu.VMEM((2, 768, 128), BF16),
        pltpu.VMEM((2, 3, 192, 128), BF16),
        pltpu.VMEM((2, 192, 128), BF16),
        pltpu.VMEM((2, 7, 32, 128), BF16),
        pltpu.VMEM((2, NY, NC, NX, 192, 128), BF16),
        pltpu.VMEM((total_adm, 256), BF16),
        pltpu.VMEM((768, 256), F32),
        pltpu.VMEM((768, 256), BF16),
        pltpu.VMEM((768, 256), F32),
        pltpu.VMEM((2, NZ, 6, 208, 128), BF16),
        pltpu.VMEM((768, 768), F32),
        pltpu.VMEM((6, 192, 384), BF16),
        pltpu.VMEM((6, 192, 384), BF16),
        pltpu.VMEM((256, 256), BF16),
        pltpu.VMEM((7, 32, 256), BF16),
        pltpu.VMEM((256, 256), BF16),
        pltpu.VMEM((2, 768, 128), BF16),
        pltpu.VMEM((2, 3, 192, 128), BF16),
        pltpu.VMEM((2, 192, 128), BF16),
        pltpu.VMEM((2, 7, 32, 128), BF16),
        pltpu.VMEM((2, NX, 192, 128), BF16),
        pltpu.VMEM((256, 640), BF16),
        pltpu.VMEM((7, 32, 640), BF16),
        pltpu.VMEM((3, 8, 128), F32),
        pltpu.VMEM((7, 8, 128), F32),
        pltpu.VMEM((3, 8, 128), F32),
        pltpu.VMEM((7, 8, 128), F32),
        pltpu.SemaphoreType.DMA((N_SEMS,)),
        pltpu.SemaphoreType.DMA((N_SEMS,)),
        pltpu.SemaphoreType.DMA((3,)),
    ]
    exchange, back, scal = pl.pallas_call(
        kernel,
        out_shape=(
            jax.ShapeDtypeStruct((out_rows, rows), F32),
            jax.ShapeDtypeStruct((32, 640), F32),
            jax.ShapeDtypeStruct((8, 128), F32),
        ),
        in_specs=[pl.BlockSpec(memory_space=pl.ANY)] * 3,
        out_specs=(vmem, vmem, vmem),
        scratch_shapes=scratch,
        compiler_params=pltpu.CompilerParams(
            collective_id=0, has_side_effects=True, vmem_limit_bytes=56 * 1024 * 1024
        ),
        name="admm_exchange",
    )(orbitals.T, projector, integrals)
    exchange, back, energy_mean, trace_mean = pl.pallas_call(
        functools.partial(finish, total_adm, nocc),
        out_shape=(
            jax.ShapeDtypeStruct((out_rows, rows), F32),
            jax.ShapeDtypeStruct((nocc // NG, npri), F32),
            jax.ShapeDtypeStruct((1, 1), F32),
            jax.ShapeDtypeStruct((1, 1), F32),
        ),
        in_specs=[vmem] * 3,
        out_specs=(vmem,) * 4,
        name="finish",
    )(exchange, back, scal)
    return exchange, back.T, energy_mean.reshape(()), trace_mean.reshape(())


def solution(mesh):
    return jax.shard_map(
        on_device,
        mesh=mesh,
        in_specs=(P("gx", None), P("gy", "gx"), P("gx", "gy", None)),
        out_specs=(P("gx", "gy"), P("gx", "gy"), P(), P()),
        check_vma=False,
    )
```
